32 devices in a mesh: outer: 2 (over core), dp: 4 (over z), tensor: 4 (over y, x).
Axes of the slice: x: 2, y: 2, z: 4, core: 2. Of those that a mesh axis runs over, the one named last changes fastest.
Arguments:
- attn: bfloat16 [2048, 8192], P(('outer', 'dp'), 'tensor'), may hold values from -6 to 6
- out_weight: bfloat16 [8192, 8192], P(None, 'tensor'), may hold values from -0.0625 to 0.0625
- resid: bfloat16 [2048, 8192], P(('outer', 'dp'), 'tensor'), may hold values from -8 to 8
- norm_gain: bfloat16 [8192], P('tensor'), may hold values from 0.5 to 1.5
- head: bfloat16 [8192], P('tensor'), may hold values from -1 to 1
- lengths: int32 [32], P(('outer', 'dp')), may hold values from 1 to 64
- pairs: int32 [32, 2], P(('outer', 'dp')), may hold values from 0 to 3, as said below
- pair_valid: int32 [32], P(('outer', 'dp')), may hold values from 0 to 1, as said below
- loss_scale: float32 [1], replicated, may hold values from 1024 to 8192
Outputs:
- loss: float32 [1], replicated
- grad_out_proj: float32 [8192, 8192], P(('outer', 'dp'), 'tensor')
- grad_gain: float32 [8192], P('tensor')
- grad_head: float32 [8192], P('tensor')
The draws below stay inside these ranges and needn't reach their ends.
Inputs may be any that keep to these rules, and one draw needn't show every extreme that they name: `pairs`: in each pair the two numbers differ; the first pair of each replica is valid. `pair_valid`: the first of each replica's 4 entries is 1.
All inputs are finite; a program needn't handle non-finite values.
Results may differ from the reference program's by a relative error of at most 0.003.
Values may be sent and summed in bfloat16 or wider, within the bound.
A program may use at most 128 MiB of HBM per device.

```python
import math
import jax
import jax.numpy as jnp
from jax import lax

D = 8192
SEQ_LEN = 64
SEQS_DEV = 4
PAIRS_DEV = 4
HD = 8192
SEQS = 32
TOKENS = 2048
PAIRS = 32


def head_vector(key):
    values = jax.random.normal(jax.random.fold_in(key, 41), (D,), jnp.float32) * (D // 16) ** (-0.5)
    return jnp.clip(values, -1.0, 1.0)


def draw_head(key, part):
    return head_vector(key).astype(jnp.bfloat16)


def draw_pairs(key, part):
    first = jax.random.randint(jax.random.fold_in(key, 11), (PAIRS,), 0, SEQS_DEV)
    step = jax.random.randint(jax.random.fold_in(key, 12), (PAIRS,), 1, SEQS_DEV)
    second = (first + step) % SEQS_DEV
    return jnp.stack([first, second], axis=1).astype(jnp.int32)


def draw_pair_valid(key, part):
    coin = jax.random.randint(jax.random.fold_in(key, 21), (PAIRS,), 0, 4)
    leading = jnp.arange(PAIRS) % PAIRS_DEV == 0
    return jnp.where(leading | (coin > 0), 1, 0).astype(jnp.int32)


def draw_resid(key, part):
    headv = head_vector(key)
    unit = headv * D ** 0.5 / jnp.sqrt(jnp.sum(headv * headv))
    rising = 0.5 * jnp.exp(jnp.log(4.0) * jnp.arange(D, dtype=jnp.float32) / D)
    rough = jax.random.uniform(jax.random.fold_in(key, 31), (D,), jnp.float32, 0.7, 1.4)
    shape = rising * rough
    base_var = jnp.mean(shape * shape)
    base = jax.random.normal(jax.random.fold_in(key, 34), (TOKENS, D), jnp.float32)
    rest = base * shape[None, :]
    spread = (base_var + 1.0) * jnp.ones((TOKENS, 1), jnp.float32)
    share = 0.3
    along = share / (1.0 - share * share) ** 0.5 * jnp.sqrt(spread)
    values = rest + along * unit[None, :]
    return jnp.clip(values, -8.0, 8.0).astype(jnp.bfloat16)


def plant(values, rng, least, high):
    longest = values.shape.index(max(values.shape))
    spots = []
    for shift in (0, 1):
        where = [jax.random.randint(jax.random.fold_in(rng, axis), (), 0, length) for axis, length in enumerate(values.shape)]
        where[longest] = (where[longest] + shift) % values.shape[longest]
        spots.append(tuple(where))
    return values.at[spots[0]].set(least).at[spots[1]].set(high)


def levels(rng, extent, shards, least, top_value):
    level, own = 1.0, jax.random.fold_in(rng, 6)
    for dim, parts in shards:
        steps = jnp.exp(jax.random.uniform(jax.random.fold_in(own, dim), (parts,), jnp.float32, least / len(shards), top_value / len(shards)))
        level = level * jnp.repeat(steps, extent[dim] // parts).reshape([-1 if axis == dim else 1 for axis in range(len(extent))])
    return level


def noise(own_key, extent, width, limit, split=(), kind=jnp.bfloat16):
    values = jax.random.normal(own_key, extent, jnp.float32) * width
    if len(split) > 0:
        values = levels(own_key, extent, split, -0.22, 0.18) * values
    return jnp.clip(values, min=-limit, max=limit).astype(kind)


def setup_inputs(seed: int = 0) -> dict:
    keys = jax.random.split(jax.random.key(seed), 10)
    attn = noise(keys[0], (TOKENS, HD), 1.0, 6.0, ((0, 8), (1, 4)))
    out_weight = noise(keys[1], (D, HD), HD ** -0.5, 0.0625, ((1, 4),))
    resid = draw_resid(jax.random.fold_in(keys[9], 71), 0)
    norm_gain = jnp.clip(1.0 + 0.1 * jax.random.normal(keys[3], (D,), jnp.float32), 0.5, 1.5).astype(jnp.bfloat16)
    head = draw_head(jax.random.fold_in(keys[9], 71), 0)
    lengths = plant(jax.random.randint(keys[5], (SEQS,), 1, SEQ_LEN + 1), jax.random.fold_in(keys[5], 1), 1, SEQ_LEN).astype(jnp.int32)
    pairs = draw_pairs(jax.random.fold_in(keys[9], 71), 0)
    pair_valid = draw_pair_valid(jax.random.fold_in(keys[9], 71), 0)
    loss_scale = jnp.clip(jnp.exp(jax.random.uniform(keys[8], (1,), jnp.float32, math.log(1024.0), math.log(8192.0))), 1024.0, 8192.0)
    return {"attn": attn, "out_weight": out_weight, "resid": resid, "norm_gain": norm_gain, "head": head, "lengths": lengths, "pairs": pairs, "pair_valid": pair_valid, "loss_scale": loss_scale}


def reference(attn, out_weight, resid, norm_gain, head, lengths, pairs, pair_valid, loss_scale):
    f32 = jnp.float32
    attn_f = attn.astype(f32)
    proj = jnp.dot(attn_f, out_weight.astype(f32).T)
    z = resid.astype(f32) + proj
    gain = norm_gain.astype(f32)
    headv = head.astype(f32)
    inv = 1.0 / jnp.sqrt(lax.optimization_barrier(jnp.mean(z * z, axis=1, keepdims=True)) + 1e-05)
    normed = z * inv * gain
    score = lax.optimization_barrier(jnp.sum(normed * headv, axis=1))
    live = (jnp.arange(SEQ_LEN)[None, :] < lengths[:, None]).astype(f32)
    lens = lengths.astype(f32)
    reward = lax.optimization_barrier(jnp.sum(score.reshape(SEQS, SEQ_LEN) * live, axis=1)) / lens
    offset = (jnp.arange(PAIRS) // PAIRS_DEV * SEQS_DEV).astype(jnp.int32)
    chosen = pairs[:, 0] + offset
    rejected = pairs[:, 1] + offset
    valid = pair_valid.astype(f32)
    margin = reward[chosen] - reward[rejected]
    count = jnp.sum(valid)
    loss = jnp.sum(valid * jax.nn.softplus(-margin)) / count
    dmargin = -loss_scale[0] * valid * jax.nn.sigmoid(-margin) / count
    dreward = jnp.zeros((SEQS,), f32).at[chosen].add(dmargin).at[rejected].add(-dmargin)
    dscore = ((dreward / lens)[:, None] * live).reshape(TOKENS)
    grad_head = lax.optimization_barrier(jnp.sum(dscore[:, None] * normed, axis=0))
    grad_gain = lax.optimization_barrier(jnp.sum(dscore[:, None] * headv * z * inv, axis=0))
    a = dscore[:, None] * headv * gain
    dproj = inv * a - z * inv ** 3 * lax.optimization_barrier(jnp.sum(a * z, axis=1, keepdims=True)) / D
    dproj = dproj.astype(jnp.bfloat16)
    grad_out_proj = jnp.dot(dproj.astype(f32).T, attn_f)
    return (loss.reshape(1), grad_out_proj, grad_gain, grad_head)
```

```python
import jax
import jax.numpy as jnp
from jax import lax
from jax.sharding import PartitionSpec as P


def shards(attn, out_weight, resid, norm_gain, head, lengths, pairs, pair_valid, loss_scale):
    f32 = jnp.float32
    tok_dev = attn.shape[0]
    feats = resid.shape[1]
    tensor = lax.axis_size("tensor")
    width = feats * tensor
    seqs_dev = lengths.shape[0]
    seq_len = tok_dev // seqs_dev
    valid = pair_valid.astype(f32)
    count = lax.psum(jnp.sum(valid), ("outer", "dp"))
    part = lax.dot_general(out_weight, attn, (((1,), (1,)), ((), ())), preferred_element_type=f32)
    part = part.astype(jnp.bfloat16).reshape(tensor, feats, tok_dev)
    part = lax.all_to_all(part, "tensor", split_axis=0, concat_axis=0, tiled=True)
    z = resid.astype(f32).T + jnp.sum(part.astype(f32), axis=0)
    gain = norm_gain.astype(f32)[:, None]
    headv = head.astype(f32)[:, None]
    both = headv * gain
    sums = lax.psum(jnp.stack([jnp.sum(z * z, axis=0), jnp.sum(z * both, axis=0)]), "tensor")
    inv = 1.0 / jnp.sqrt(sums[0] / width + 1e-05)
    score = sums[1] * inv
    position = jnp.arange(tok_dev)
    seq_of = position // seq_len
    within = position % seq_len
    member = (within[:, None] < lengths[None, :]) & (
        seq_of[:, None] == jnp.arange(seqs_dev)[None, :]
    )
    pooling = member.astype(f32) / lengths.astype(f32)[None, :]
    reward = jnp.sum(pooling * score[:, None], axis=0)
    choose = jnp.arange(seqs_dev)[None, :]
    select = (pairs[:, 0:1] == choose).astype(f32) - (pairs[:, 1:2] == choose).astype(f32)
    margin = jnp.sum(select * reward[None, :], axis=1)
    loss_part = jnp.sum(valid * jax.nn.softplus(-margin))
    dmargin = -loss_scale[0] * valid * jax.nn.sigmoid(-margin) / count
    dreward = jnp.sum(dmargin[:, None] * select, axis=0)
    dscore = jnp.sum(pooling * dreward[None, :], axis=1)
    weight = inv * dscore
    dproj = weight[None, :] * both - z * (inv**3 * dscore * sums[1] / width)[None, :]
    dproj = dproj.astype(jnp.bfloat16)
    zsum = jnp.sum(z * weight[None, :], axis=1)
    gathered = lax.all_gather(dproj, "tensor", axis=0, tiled=True)
    exchanged = lax.all_to_all(gathered, ("outer", "dp"), split_axis=0, concat_axis=1, tiled=True)
    grad_out_proj = jnp.dot(
        exchanged,
        lax.all_gather(attn, ("outer", "dp"), axis=0, tiled=True),
        preferred_element_type=f32,
    )
    zsum, loss_sum = lax.psum((zsum, loss_part), ("outer", "dp"))
    loss = (loss_sum / count).reshape(1)
    return (loss, grad_out_proj, zsum * headv[:, 0], zsum * gain[:, 0])


def solution(mesh):
    return jax.shard_map(
        shards,
        mesh=mesh,
        in_specs=(
            P(("outer", "dp"), "tensor"),
            P(None, "tensor"),
            P(("outer", "dp"), "tensor"),
            P("tensor"),
            P("tensor"),
            P(("outer", "dp")),
            P(("outer", "dp"), None),
            P(("outer", "dp")),
            P(),
        ),
        out_specs=(P(), P(("outer", "dp"), "tensor"), P("tensor"), P("tensor")),
        check_vma=False,
    )
```

```python
import functools

import jax
import jax.numpy as jnp
from jax import lax
from jax.experimental import pallas as pl
from jax.experimental.pallas import tpu as pltpu
from jax.sharding import PartitionSpec as P

MESH = pl.DeviceIdType.MESH
F32 = jnp.float32
BF16 = jnp.bfloat16
SLOTS = 3


def bits_of(count):
    return count.bit_length() - 1


def flip(index, mask, bits):
    out = 0
    for j in range(bits):
        out = out + ((index // 2**j + mask // 2**j) % 2) * 2**j
    return out


def kernel(
    sizes,
    attn,
    weight,
    resid,
    both,
    pool,
    select,
    scaled_valid,
    valid,
    vsum,
    exch,
    attn_all,
    qtot,
    ltot,
    ctot,
    wbuf,
    attn_t,
    part,
    got,
    z,
    dp,
    stat,
    stat_in,
    cin,
    lsrc,
    lin,
    qsrc,
    qin,
    wsem,
    rs_send,
    rs_recv,
    st_send,
    st_recv,
    c_send,
    c_recv,
    l_send,
    l_recv,
    q_send,
    q_recv,
    ag_local,
    ag_right,
    ag_left,
    ag_out,
    ag_recv,
    z_send,
    b_send,
    e_recv,
):
    T, O, Z = sizes
    N = O * Z
    bits = bits_of(T)
    R = N // T
    tok, feats = resid.shape
    width = feats * T
    blk = width // N
    tile = wbuf.shape[1]
    per = feats // tile
    o, p, t = lax.axis_index("outer"), lax.axis_index("dp"), lax.axis_index("tensor")
    me = o * Z + p

    def replica(k):
        return (k // Z, k % Z, t)

    def tensor_peer(r):
        return (o, p, flip(t, r, bits))

    barrier = pltpu.get_barrier_semaphore()
    for r in range(1, T):
        pl.semaphore_signal(barrier, inc=1, device_id=tensor_peer(r), device_id_type=MESH)
    for d in range(1, N):
        pl.semaphore_signal(barrier, inc=1, device_id=replica((me + d) % N), device_id_type=MESH)

    def load(i):
        target = flip(t, T - 1 - i // per, bits)
        start = pl.multiple_of(target * feats + (i % per) * tile, tile)
        return pltpu.make_async_copy(
            weight.at[pl.ds(start, tile)], wbuf.at[i % SLOTS], wsem.at[i % SLOTS]
        )

    for i in range(min(SLOTS - 1, T * per)):
        load(i).start()

    def turn_attn(c, carry):
        cols = pl.ds(pl.multiple_of(c * 128, 128), 128)
        attn_t[cols, :] = attn[:, cols].astype(F32).T.astype(BF16)
        return carry

    lax.fori_loop(0, feats // 128, turn_attn, 0)
    pl.semaphore_wait(barrier, T - 1 + N - 1)

    def peer_copy(src, dst, send, recv, d):
        return pltpu.make_async_remote_copy(
            src_ref=src,
            dst_ref=dst.at[d],
            send_sem=send.at[d],
            recv_sem=recv.at[d],
            device_id=replica((me + d) % N),
            device_id_type=MESH,
        )

    def block_rows(outer, b):
        return pl.ds(pl.multiple_of((outer * Z + b) * tok, tok), tok)

    def ag_copy(src, b, send, where):
        return pltpu.make_async_remote_copy(
            src_ref=src,
            dst_ref=attn_all.at[block_rows(o, b)],
            send_sem=send,
            recv_sem=ag_recv.at[o, b],
            device_id=where,
            device_id_type=MESH,
        )

    def right_copy(s):
        b = (p + Z - s) % Z
        src = attn if s == 0 else attn_all.at[block_rows(o, b)]
        return ag_copy(src, b, ag_right.at[s], (o, (p + 1) % Z, t))

    def left_copy(s):
        b = (p + s) % Z
        src = attn if s == 0 else attn_all.at[block_rows(o, b)]
        return ag_copy(src, b, ag_left.at[s], (o, (p + Z - 1) % Z, t))

    def right_sends(s):
        return (p >= s) & (p < Z - 1)

    def left_sends(s):
        return (p + s < Z) & (p > 0)

    def out_copy(b, e, own=False):
        src = attn if own else attn_all.at[block_rows(o, b)]
        return ag_copy(src, b, ag_out.at[e, b], ((o + e) % O, p, t))

    def arrived(outer, b):
        rows = attn_all.at[block_rows(outer, b)]
        return pltpu.make_async_remote_copy(
            src_ref=rows,
            dst_ref=rows,
            send_sem=ag_out.at[0, 0],
            recv_sem=ag_recv.at[outer, b],
            device_id=(o, (p + 1) % Z, t),
            device_id_type=MESH,
        )

    def arrival(s):
        for ok, b in ((p - 1 - s >= 0, (p + Z - 1 - s) % Z), (p + 1 + s < Z, (p + 1 + s) % Z)):

            @pl.when(ok)
            def _():
                arrived(o, b).wait_recv()
                for e in range(1, O):
                    out_copy(b, e).start()

        if s + 1 < Z - 1:
            for ok, copy in ((right_sends(s + 1), right_copy), (left_sends(s + 1), left_copy)):

                @pl.when(ok)
                def _():
                    copy(s + 1).start()

    for ok, copy in ((right_sends(0), right_copy), (left_sends(0), left_copy)):

        @pl.when(ok)
        def _():
            copy(0).start()

    for e in range(1, O):
        out_copy(p, e, True).start()
    own_rows = pltpu.make_async_copy(attn, attn_all.at[block_rows(o, p)], ag_local)
    own_rows.start()
    for d in range(1, N):
        peer_copy(vsum, cin, c_send, c_recv, d).start()

    def rs_copy(r, j):
        return pltpu.make_async_remote_copy(
            src_ref=part.at[r, j],
            dst_ref=got.at[r, j],
            send_sem=rs_send.at[r, j],
            recv_sem=rs_recv.at[r, j],
            device_id=tensor_peer(r),
            device_id_type=MESH,
        )

    def project(i, carry):
        @pl.when(i + SLOTS - 1 < T * per)
        def _():
            load(i + SLOTS - 1).start()

        load(i).wait()
        r, j = T - 1 - i // per, i % per
        part[r, j] = jnp.dot(
            wbuf[i % SLOTS], attn_t[...], preferred_element_type=F32
        ).astype(BF16)

        @pl.when(r > 0)
        def _():
            rs_copy(r, j).start()

        return carry

    lax.fori_loop(0, T * per, project, 0)

    def rows_of(j):
        return pl.ds(pl.multiple_of(j * tile, tile), tile)

    def turn_resid(j, carry):
        z[rows_of(j), :] = resid[:, rows_of(j)].astype(F32).T + part[0, j].astype(F32)
        return carry

    lax.fori_loop(0, per, turn_resid, 0)
    arrival(0)

    def gather_z(j, carry):
        squares, heads = carry
        total = z[rows_of(j), :]
        for r in range(T - 1, 0, -1):
            rs_copy(r, j).wait_recv()
            total = total + got[r, j].astype(F32)
        z[rows_of(j), :] = total
        squares = squares + jnp.sum(total * total, axis=0, keepdims=True)
        heads = heads + jnp.sum(total * both[rows_of(j), :], axis=0, keepdims=True)
        return squares, heads

    zero = jnp.zeros((1, tok), F32)
    squares, heads = lax.fori_loop(0, per, gather_z, (zero, zero))
    stat[0:1, :] = squares
    stat[1:2, :] = heads

    def stat_copy(r):
        return pltpu.make_async_remote_copy(
            src_ref=stat,
            dst_ref=stat_in.at[r],
            send_sem=st_send.at[r],
            recv_sem=st_recv.at[r],
            device_id=tensor_peer(r),
            device_id_type=MESH,
        )

    for r in range(1, T):
        stat_copy(r).start()
    count = vsum[0:1, 0:1]
    for d in range(1, N):
        peer_copy(vsum, cin, c_send, c_recv, d).wait_recv()
        count = count + cin[d, 0:1, 0:1]
    if Z > 2:
        arrival(1)
    for r in range(1, T):
        stat_copy(r).wait_recv()
        squares = squares + stat_in[r, 0:1, :]
        heads = heads + stat_in[r, 1:2, :]
    inv = 1.0 / jnp.sqrt(squares / width + 1e-05)
    score = heads * inv
    reward = jnp.sum(pool[...] * score, axis=1, keepdims=True)
    margin = jnp.sum(select[...] * reward, axis=0, keepdims=True)
    soft = jnp.maximum(-margin, 0.0) + jnp.log1p(jnp.exp(-jnp.abs(margin)))
    loss = jnp.sum(valid[...] * soft, axis=1, keepdims=True)
    dmargin = scaled_valid[...] * jax.nn.sigmoid(-margin) / count
    dreward = jnp.sum(select[...] * dmargin, axis=1, keepdims=True)
    dscore = jnp.sum(pool[...] * dreward, axis=0, keepdims=True)
    scale = inv * dscore
    pull = inv * inv * inv * dscore * heads / width

    def make_dproj(j, carry):
        rows = rows_of(j)
        dp[rows, :] = (scale * both[rows, :] - z[rows, :] * pull).astype(BF16)
        return carry

    lax.fori_loop(0, per, make_dproj, 0)

    def cols_of(k):
        return exch.at[:, pl.ds(pl.multiple_of(k * tok, tok), tok)]

    def piece(j):
        return dp.at[pl.ds(j * blk, blk)]

    def piece_copy(j):
        return pltpu.make_async_remote_copy(
            src_ref=piece(j),
            dst_ref=cols_of(me),
            send_sem=z_send.at[j],
            recv_sem=e_recv.at[me],
            device_id=replica(t * R + j),
            device_id_type=MESH,
        )

    def piece_local(j):
        return pltpu.make_async_copy(piece(j), cols_of(me), e_recv.at[me])

    for j in range(R):

        @pl.when(t * R + j != me)
        def _():
            piece_copy(j).start()

        @pl.when(t * R + j == me)
        def _():
            piece_local(j).start()

    lsrc[...] = jnp.broadcast_to(loss, lsrc.shape)
    for j in range(per):
        rows = pl.ds(j * tile, tile)
        zw = z[rows, :] * scale
        lanes = zw[:, 0:128]
        for h in range(1, tok // 128):
            lanes = lanes + zw[:, h * 128 : (h + 1) * 128]
        qsrc[0:1, j * tile : (j + 1) * tile] = jnp.sum(lanes.T, axis=0, keepdims=True)
    for d in range(1, N):
        peer_copy(lsrc, lin, l_send, l_recv, d).start()
        peer_copy(qsrc, qin, q_send, q_recv, d).start()

    owner = me // R
    rank = flip(t, owner, bits)
    step = 1 + (p // (Z - Z // 2)) * (Z - 2)

    def child_copy(j, k):
        return pltpu.make_async_remote_copy(
            src_ref=cols_of(k),
            dst_ref=cols_of(k),
            send_sem=b_send.at[j, k],
            recv_sem=e_recv.at[k],
            device_id=tensor_peer(2**j),
            device_id_type=MESH,
        )

    def spread(i, carry):
        k = ((o + i) % O) * Z + (p + step * (i // O)) % Z
        child_copy(0, k).wait_recv()
        for j in range(bits):

            @pl.when(rank < 2**j)
            def _():
                child_copy(j, k).start()

        return carry

    lax.fori_loop(0, N // 2, spread, 0)
    for s in range(2, Z - 1):
        arrival(s)
    lax.fori_loop(N // 2, N, spread, 0)
    if Z == 2:
        pass

    ltotal, qtotal = lsrc[...], qsrc[...]
    for d in range(1, N):
        peer_copy(lsrc, lin, l_send, l_recv, d).wait_recv()
        peer_copy(qsrc, qin, q_send, q_recv, d).wait_recv()
        ltotal = ltotal + lin[d]
        qtotal = qtotal + qin[d]
    ltot[...] = ltotal
    qtot[...] = qtotal
    ctot[...] = jnp.broadcast_to(count, ctot.shape)

    for e in range(1, O):
        for b in range(Z):
            arrived((o + e) % O, b).wait_recv()
    own_rows.wait()
    for s in range(Z - 1):
        for ok, copy in ((right_sends(s), right_copy), (left_sends(s), left_copy)):

            @pl.when(ok)
            def _():
                copy(s).wait_send()

    for e in range(1, O):
        for b in range(Z):
            out_copy(b, e).wait_send()
    for d in range(1, N):
        peer_copy(vsum, cin, c_send, c_recv, d).wait_send()
        peer_copy(lsrc, lin, l_send, l_recv, d).wait_send()
        peer_copy(qsrc, qin, q_send, q_recv, d).wait_send()
    for r in range(1, T):
        stat_copy(r).wait_send()
        for j in range(per):
            rs_copy(r, j).wait_send()
    for j in range(R):

        @pl.when(t * R + j != me)
        def _():
            piece_copy(j).wait_send()

    def spread_end(k, carry):
        for j in range(bits):

            @pl.when(rank < 2**j)
            def _():
                child_copy(j, k).wait_send()

        return carry

    lax.fori_loop(0, N, spread_end, 0)


def shards(sizes, attn, out_weight, resid, norm_gain, head, lengths, pairs, pair_valid, loss_scale):
    T, O, Z = sizes
    N = O * Z
    tok, feats = resid.shape
    width = feats * T
    blk = width // N
    heads_dev = attn.shape[1]
    tile = min(512, feats)
    per = feats // tile
    seqs_dev = lengths.shape[0]
    seq_len = tok // seqs_dev
    valid = pair_valid.astype(F32)
    gain = norm_gain.astype(F32)
    headv = head.astype(F32)
    position = jnp.arange(tok)[None, :]
    mine = jnp.arange(seqs_dev)[:, None]
    member = (position % seq_len < lengths[:, None]) & (position // seq_len == mine)
    pool = member.astype(F32) / lengths.astype(F32)[:, None]
    select = (pairs[:, 0][None, :] == mine).astype(F32) - (pairs[:, 1][None, :] == mine).astype(F32)
    vsum = jnp.broadcast_to(jnp.sum(valid), (8, 128))
    vmem = pl.BlockSpec(memory_space=pltpu.VMEM)
    anyw = pl.BlockSpec(memory_space=pl.ANY)
    sem = pltpu.SemaphoreType.DMA
    bits = bits_of(T)
    exch, attn_all, qtot, ltot, ctot = pl.pallas_call(
        functools.partial(kernel, sizes),
        out_shape=(
            jax.ShapeDtypeStruct((blk, N * tok), BF16),
            jax.ShapeDtypeStruct((N * tok, heads_dev), BF16),
            jax.ShapeDtypeStruct((1, feats), F32),
            jax.ShapeDtypeStruct((8, 128), F32),
            jax.ShapeDtypeStruct((8, 128), F32),
        ),
        in_specs=[vmem, anyw, vmem, vmem, vmem, vmem, vmem, vmem, vmem],
        out_specs=(anyw, anyw, vmem, vmem, vmem),
        scratch_shapes=[
            pltpu.VMEM((SLOTS, tile, heads_dev), BF16),
            pltpu.VMEM((heads_dev, tok), BF16),
            pltpu.VMEM((T, per, tile, tok), BF16),
            pltpu.VMEM((T, per, tile, tok), BF16),
            pltpu.VMEM((feats, tok), F32),
            pltpu.VMEM((feats, tok), BF16),
            pltpu.VMEM((2, tok), F32),
            pltpu.VMEM((T, 2, tok), F32),
            pltpu.VMEM((N, 8, 128), F32),
            pltpu.VMEM((8, 128), F32),
            pltpu.VMEM((N, 8, 128), F32),
            pltpu.VMEM((1, feats), F32),
            pltpu.VMEM((N, 1, feats), F32),
            sem((SLOTS,)),
            sem((T, per)),
            sem((T, per)),
            sem((T,)),
            sem((T,)),
            sem((N,)),
            sem((N,)),
            sem((N,)),
            sem((N,)),
            sem((N,)),
            sem((N,)),
            sem,
            sem((Z,)),
            sem((Z,)),
            sem((O, Z)),
            sem((O, Z)),
            sem((N // T,)),
            sem((bits, N)),
            sem((N,)),
        ],
        compiler_params=pltpu.CompilerParams(
            collective_id=0, has_side_effects=True, vmem_limit_bytes=60 * 1024 * 1024
        ),
    )(
        attn,
        out_weight,
        resid,
        (gain * headv)[:, None],
        pool,
        select,
        (-loss_scale[0] * valid)[None, :],
        valid[None, :],
        vsum,
    )
    grad_out_proj = jnp.dot(exch, attn_all, preferred_element_type=F32)
    loss = (ltot[0, 0] / ctot[0, 0]).reshape(1)
    return (loss, grad_out_proj, qtot[0] * headv, qtot[0] * gain)


def solution(mesh):
    sizes = (mesh.shape["tensor"], mesh.shape["outer"], mesh.shape["dp"])
    return jax.shard_map(
        functools.partial(shards, sizes),
        mesh=mesh,
        in_specs=(
            P(("outer", "dp"), "tensor"),
            P(None, "tensor"),
            P(("outer", "dp"), "tensor"),
            P("tensor"),
            P("tensor"),
            P(("outer", "dp")),
            P(("outer", "dp"), None),
            P(("outer", "dp")),
            P(),
        ),
        out_specs=(P(), P(("outer", "dp"), "tensor"), P("tensor"), P("tensor")),
        check_vma=False,
    )
```

```python
import functools

import jax
import jax.numpy as jnp
from jax import lax
from jax.experimental import pallas as pl
from jax.experimental.pallas import tpu as pltpu
from jax.sharding import PartitionSpec as P

MESH = pl.DeviceIdType.MESH
F32 = jnp.float32
BF16 = jnp.bfloat16
SLOTS = 3


def bits_of(count):
    return count.bit_length() - 1


def flip(index, mask, bits):
    out = 0
    for j in range(bits):
        out = out + ((index // 2**j + mask // 2**j) % 2) * 2**j
    return out


def kernel(
    sizes,
    attn,
    weight,
    resid,
    both,
    pool,
    select,
    scaled_valid,
    valid,
    vsum,
    grad,
    qtot,
    ltot,
    ctot,
    exch,
    attn_all,
    acc,
    wbuf,
    attn_t,
    part,
    got,
    z,
    dp,
    stat,
    stat_in,
    cin,
    lsrc,
    lin,
    qsrc,
    qin,
    wsem,
    rs_send,
    rs_recv,
    st_send,
    st_recv,
    c_send,
    c_recv,
    l_send,
    l_recv,
    q_send,
    q_recv,
    ag_local,
    ag_right,
    ag_left,
    ag_out,
    ag_recv,
    z_send,
    b_send,
    e_recv,
    o_sem,
):
    T, O, Z = sizes
    N = O * Z
    bits = bits_of(T)
    R = N // T
    tok, feats = resid.shape
    width = feats * T
    blk = width // N
    tile = wbuf.shape[1]
    per = feats // tile
    o, p, t = lax.axis_index("outer"), lax.axis_index("dp"), lax.axis_index("tensor")
    me = o * Z + p

    def replica(k):
        return (k // Z, k % Z, t)

    def tensor_peer(r):
        return (o, p, flip(t, r, bits))

    barrier = pltpu.get_barrier_semaphore()
    for r in range(1, T):
        pl.semaphore_signal(barrier, inc=1, device_id=tensor_peer(r), device_id_type=MESH)
    for d in range(1, N):
        pl.semaphore_signal(barrier, inc=1, device_id=replica((me + d) % N), device_id_type=MESH)

    def load(i):
        target = flip(t, T - 1 - i // per, bits)
        start = pl.multiple_of(target * feats + (i % per) * tile, tile)
        return pltpu.make_async_copy(
            weight.at[pl.ds(start, tile)], wbuf.at[i % SLOTS], wsem.at[i % SLOTS]
        )

    for i in range(min(SLOTS - 1, T * per)):
        load(i).start()

    def turn_attn(c, carry):
        cols = pl.ds(pl.multiple_of(c * 128, 128), 128)
        attn_t[cols, :] = attn[:, cols].astype(F32).T.astype(BF16)
        return carry

    lax.fori_loop(0, feats // 128, turn_attn, 0)
    pl.semaphore_wait(barrier, T - 1 + N - 1)

    def peer_copy(src, dst, send, recv, d):
        return pltpu.make_async_remote_copy(
            src_ref=src,
            dst_ref=dst.at[d],
            send_sem=send.at[d],
            recv_sem=recv.at[d],
            device_id=replica((me + d) % N),
            device_id_type=MESH,
        )

    def block_rows(outer, b):
        return outer * Z + b

    def ag_copy(src, b, send, where):
        return pltpu.make_async_remote_copy(
            src_ref=src,
            dst_ref=attn_all.at[block_rows(o, b)],
            send_sem=send,
            recv_sem=ag_recv.at[o, b],
            device_id=where,
            device_id_type=MESH,
        )

    def right_copy(s):
        b = (p + Z - s) % Z
        src = attn if s == 0 else attn_all.at[block_rows(o, b)]
        return ag_copy(src, b, ag_right.at[s], (o, (p + 1) % Z, t))

    def left_copy(s):
        b = (p + s) % Z
        src = attn if s == 0 else attn_all.at[block_rows(o, b)]
        return ag_copy(src, b, ag_left.at[s], (o, (p + Z - 1) % Z, t))

    def right_sends(s):
        return (p >= s) & (p < Z - 1)

    def left_sends(s):
        return (p + s < Z) & (p > 0)

    def out_copy(b, e, own=False):
        src = attn if own else attn_all.at[block_rows(o, b)]
        return ag_copy(src, b, ag_out.at[e, b], ((o + e) % O, p, t))

    def arrived(outer, b):
        rows = attn_all.at[block_rows(outer, b)]
        return pltpu.make_async_remote_copy(
            src_ref=rows,
            dst_ref=rows,
            send_sem=ag_out.at[0, 0],
            recv_sem=ag_recv.at[outer, b],
            device_id=(o, (p + 1) % Z, t),
            device_id_type=MESH,
        )

    def arrival(s):
        for ok, b in ((p - 1 - s >= 0, (p + Z - 1 - s) % Z), (p + 1 + s < Z, (p + 1 + s) % Z)):

            @pl.when(ok)
            def _():
                arrived(o, b).wait_recv()
                for e in range(1, O):
                    out_copy(b, e).start()

        if s + 1 < Z - 1:
            for ok, copy in ((right_sends(s + 1), right_copy), (left_sends(s + 1), left_copy)):

                @pl.when(ok)
                def _():
                    copy(s + 1).start()

    for ok, copy in ((right_sends(0), right_copy), (left_sends(0), left_copy)):

        @pl.when(ok)
        def _():
            copy(0).start()

    for e in range(1, O):
        out_copy(p, e, True).start()
    own_rows = pltpu.make_async_copy(attn, attn_all.at[block_rows(o, p)], ag_local)
    own_rows.start()
    for d in range(1, N):
        peer_copy(vsum, cin, c_send, c_recv, d).start()

    def rs_copy(r, j):
        return pltpu.make_async_remote_copy(
            src_ref=part.at[r, j],
            dst_ref=got.at[r, j],
            send_sem=rs_send.at[r, j],
            recv_sem=rs_recv.at[r, j],
            device_id=tensor_peer(r),
            device_id_type=MESH,
        )

    def project(i, carry):
        @pl.when(i + SLOTS - 1 < T * per)
        def _():
            load(i + SLOTS - 1).start()

        load(i).wait()
        r, j = T - 1 - i // per, i % per
        part[r, j] = jnp.dot(
            wbuf[i % SLOTS], attn_t[...], preferred_element_type=F32
        ).astype(BF16)

        @pl.when(r > 0)
        def _():
            rs_copy(r, j).start()

        return carry

    lax.fori_loop(0, T * per, project, 0)

    def rows_of(j):
        return pl.ds(pl.multiple_of(j * tile, tile), tile)

    def turn_resid(j, carry):
        z[rows_of(j), :] = resid[:, rows_of(j)].astype(F32).T + part[0, j].astype(F32)
        return carry

    lax.fori_loop(0, per, turn_resid, 0)

    def clear(j, carry):
        acc[pl.ds(pl.multiple_of(j * 128, 128), 128), :] = jnp.zeros((128, acc.shape[1]), F32)
        return carry

    lax.fori_loop(0, blk // 128, clear, 0)
    arrival(0)

    def gather_z(j, carry):
        squares, heads = carry
        total = z[rows_of(j), :]
        for r in range(T - 1, 0, -1):
            rs_copy(r, j).wait_recv()
            total = total + got[r, j].astype(F32)
        z[rows_of(j), :] = total
        squares = squares + jnp.sum(total * total, axis=0, keepdims=True)
        heads = heads + jnp.sum(total * both[rows_of(j), :], axis=0, keepdims=True)
        return squares, heads

    zero = jnp.zeros((1, tok), F32)
    squares, heads = lax.fori_loop(0, per, gather_z, (zero, zero))
    stat[0:1, :] = squares
    stat[1:2, :] = heads

    def stat_copy(r):
        return pltpu.make_async_remote_copy(
            src_ref=stat,
            dst_ref=stat_in.at[r],
            send_sem=st_send.at[r],
            recv_sem=st_recv.at[r],
            device_id=tensor_peer(r),
            device_id_type=MESH,
        )

    for r in range(1, T):
        stat_copy(r).start()
    count = vsum[0:1, 0:1]
    for d in range(1, N):
        peer_copy(vsum, cin, c_send, c_recv, d).wait_recv()
        count = count + cin[d, 0:1, 0:1]
    if Z > 2:
        arrival(1)
    for r in range(1, T):
        stat_copy(r).wait_recv()
        squares = squares + stat_in[r, 0:1, :]
        heads = heads + stat_in[r, 1:2, :]
    inv = 1.0 / jnp.sqrt(squares / width + 1e-05)
    score = heads * inv
    reward = jnp.sum(pool[...] * score, axis=1, keepdims=True)
    margin = jnp.sum(select[...] * reward, axis=0, keepdims=True)
    soft = jnp.maximum(-margin, 0.0) + jnp.log1p(jnp.exp(-jnp.abs(margin)))
    loss = jnp.sum(valid[...] * soft, axis=1, keepdims=True)
    dmargin = scaled_valid[...] * jax.nn.sigmoid(-margin) / count
    dreward = jnp.sum(select[...] * dmargin, axis=1, keepdims=True)
    dscore = jnp.sum(pool[...] * dreward, axis=0, keepdims=True)
    scale = inv * dscore
    pull = inv * inv * inv * dscore * heads / width

    def make_dproj(j, carry):
        rows = rows_of(j)
        dp[rows, :] = (scale * both[rows, :] - z[rows, :] * pull).astype(BF16)
        return carry

    lax.fori_loop(0, per, make_dproj, 0)

    def cols_of(k):
        return exch.at[k]

    def piece(j):
        return dp.at[pl.ds(j * blk, blk)]

    def piece_copy(j):
        return pltpu.make_async_remote_copy(
            src_ref=piece(j),
            dst_ref=cols_of(me),
            send_sem=z_send.at[j],
            recv_sem=e_recv.at[me],
            device_id=replica(t * R + j),
            device_id_type=MESH,
        )

    def piece_local(j):
        return pltpu.make_async_copy(piece(j), cols_of(me), e_recv.at[me])

    for j in range(R):

        @pl.when(t * R + j != me)
        def _():
            piece_copy(j).start()

        @pl.when(t * R + j == me)
        def _():
            piece_local(j).start()

    lsrc[...] = jnp.broadcast_to(loss, lsrc.shape)
    for j in range(per):
        rows = pl.ds(j * tile, tile)
        zw = z[rows, :] * scale
        lanes = zw[:, 0:128]
        for h in range(1, tok // 128):
            lanes = lanes + zw[:, h * 128 : (h + 1) * 128]
        qsrc[0:1, j * tile : (j + 1) * tile] = jnp.sum(lanes.T, axis=0, keepdims=True)
    for d in range(1, N):
        peer_copy(lsrc, lin, l_send, l_recv, d).start()
        peer_copy(qsrc, qin, q_send, q_recv, d).start()

    owner = me // R
    rank = flip(t, owner, bits)
    step = 1 + (p // (Z - Z // 2)) * (Z - 2)

    def child_copy(j, k):
        return pltpu.make_async_remote_copy(
            src_ref=cols_of(k),
            dst_ref=cols_of(k),
            send_sem=b_send.at[j, k],
            recv_sem=e_recv.at[k],
            device_id=tensor_peer(2**j),
            device_id_type=MESH,
        )

    def place(i):
        return (o + i) % O, (p + step * (i // O)) % Z

    def forward(i):
        outer, b = place(i)
        k = outer * Z + b
        child_copy(0, k).wait_recv()
        for j in range(bits):

            @pl.when(rank < 2**j)
            def _():
                child_copy(j, k).start()

    wide = min(512, acc.shape[1])
    strips = acc.shape[1] // wide

    def strip(c):
        return pl.ds(pl.multiple_of(c * wide, wide), wide)

    def out_strip(c):
        return pltpu.make_async_copy(acc.at[:, strip(c)], grad.at[:, strip(c)], o_sem.at[c])

    def multiply(i):
        outer, b = place(i)
        k = outer * Z + b

        @pl.when(i % O > 0)
        def _():
            arrived(outer, b).wait_recv()

        def one(c, carry):
            acc[:, strip(c)] += jnp.dot(
                exch[k], attn_all[k, :, strip(c)], preferred_element_type=F32
            )

            @pl.when(i == N - 1)
            def _():
                out_strip(c).start()

            return carry

        lax.fori_loop(0, strips, one, 0)

    def first_half(i, carry):
        forward(i)
        return carry

    def second_half(i, carry):
        forward(i)

        def both_halves(h, inner):
            multiply(i - N // 2 + h * (N // 2))
            return inner

        return lax.fori_loop(0, 2, both_halves, carry)

    own_rows.wait()
    lax.fori_loop(0, N // 2, first_half, 0)
    for s in range(2, Z - 1):
        arrival(s)
    lax.fori_loop(N // 2, N, second_half, 0)

    ltotal, qtotal = lsrc[...], qsrc[...]
    for d in range(1, N):
        peer_copy(lsrc, lin, l_send, l_recv, d).wait_recv()
        peer_copy(qsrc, qin, q_send, q_recv, d).wait_recv()
        ltotal = ltotal + lin[d]
        qtotal = qtotal + qin[d]
    ltot[...] = ltotal
    qtot[...] = qtotal
    ctot[...] = jnp.broadcast_to(count, ctot.shape)

    for s in range(Z - 1):
        for ok, copy in ((right_sends(s), right_copy), (left_sends(s), left_copy)):

            @pl.when(ok)
            def _():
                copy(s).wait_send()

    for e in range(1, O):
        for b in range(Z):
            out_copy(b, e).wait_send()
    for d in range(1, N):
        peer_copy(vsum, cin, c_send, c_recv, d).wait_send()
        peer_copy(lsrc, lin, l_send, l_recv, d).wait_send()
        peer_copy(qsrc, qin, q_send, q_recv, d).wait_send()
    for r in range(1, T):
        stat_copy(r).wait_send()
        for j in range(per):
            rs_copy(r, j).wait_send()
    for j in range(R):

        @pl.when(t * R + j != me)
        def _():
            piece_copy(j).wait_send()

    def spread_end(k, carry):
        for j in range(bits):

            @pl.when(rank < 2**j)
            def _():
                child_copy(j, k).wait_send()

        return carry

    lax.fori_loop(0, N, spread_end, 0)
    for c in range(strips):
        out_strip(c).wait()


def shards(sizes, attn, out_weight, resid, norm_gain, head, lengths, pairs, pair_valid, loss_scale):
    T, O, Z = sizes
    N = O * Z
    tok, feats = resid.shape
    width = feats * T
    blk = width // N
    heads_dev = attn.shape[1]
    tile = min(512, feats)
    per = feats // tile
    seqs_dev = lengths.shape[0]
    seq_len = tok // seqs_dev
    valid = pair_valid.astype(F32)
    gain = norm_gain.astype(F32)
    headv = head.astype(F32)
    position = jnp.arange(tok)[None, :]
    mine = jnp.arange(seqs_dev)[:, None]
    member = (position % seq_len < lengths[:, None]) & (position // seq_len == mine)
    pool = member.astype(F32) / lengths.astype(F32)[:, None]
    select = (pairs[:, 0][None, :] == mine).astype(F32) - (pairs[:, 1][None, :] == mine).astype(F32)
    vsum = jnp.broadcast_to(jnp.sum(valid), (8, 128))
    vmem = pl.BlockSpec(memory_space=pltpu.VMEM)
    anyw = pl.BlockSpec(memory_space=pl.ANY)
    sem = pltpu.SemaphoreType.DMA
    bits = bits_of(T)
    grad_out_proj, qtot, ltot, ctot = pl.pallas_call(
        functools.partial(kernel, sizes),
        out_shape=(
            jax.ShapeDtypeStruct((blk, heads_dev), F32),
            jax.ShapeDtypeStruct((1, feats), F32),
            jax.ShapeDtypeStruct((8, 128), F32),
            jax.ShapeDtypeStruct((8, 128), F32),
        ),
        in_specs=[vmem, anyw, vmem, vmem, vmem, vmem, vmem, vmem, vmem],
        out_specs=(anyw, vmem, vmem, vmem),
        scratch_shapes=[
            pltpu.VMEM((N, blk, tok), BF16),
            pltpu.VMEM((N, tok, heads_dev), BF16),
            pltpu.VMEM((blk, heads_dev), F32),
            pltpu.VMEM((SLOTS, tile, heads_dev), BF16),
            pltpu.VMEM((heads_dev, tok), BF16),
            pltpu.VMEM((T, per, tile, tok), BF16),
            pltpu.VMEM((T, per, tile, tok), BF16),
            pltpu.VMEM((feats, tok), F32),
            pltpu.VMEM((feats, tok), BF16),
            pltpu.VMEM((2, tok), F32),
            pltpu.VMEM((T, 2, tok), F32),
            pltpu.VMEM((N, 8, 128), F32),
            pltpu.VMEM((8, 128), F32),
            pltpu.VMEM((N, 8, 128), F32),
            pltpu.VMEM((1, feats), F32),
            pltpu.VMEM((N, 1, feats), F32),
            sem((SLOTS,)),
            sem((T, per)),
            sem((T, per)),
            sem((T,)),
            sem((T,)),
            sem((N,)),
            sem((N,)),
            sem((N,)),
            sem((N,)),
            sem((N,)),
            sem((N,)),
            sem,
            sem((Z,)),
            sem((Z,)),
            sem((O, Z)),
            sem((O, Z)),
            sem((N // T,)),
            sem((bits, N)),
            sem((N,)),
            sem((heads_dev // min(512, heads_dev),)),
        ],
        compiler_params=pltpu.CompilerParams(
            collective_id=0, has_side_effects=True, vmem_limit_bytes=60 * 1024 * 1024
        ),
    )(
        attn,
        out_weight,
        resid,
        (gain * headv)[:, None],
        pool,
        select,
        (-loss_scale[0] * valid)[None, :],
        valid[None, :],
        vsum,
    )
    loss = (ltot[0, 0] / ctot[0, 0]).reshape(1)
    return (loss, grad_out_proj, qtot[0] * headv, qtot[0] * gain)


def solution(mesh):
    sizes = (mesh.shape["tensor"], mesh.shape["outer"], mesh.shape["dp"])
    return jax.shard_map(
        functools.partial(shards, sizes),
        mesh=mesh,
        in_specs=(
            P(("outer", "dp"), "tensor"),
            P(None, "tensor"),
            P(("outer", "dp"), "tensor"),
            P("tensor"),
            P("tensor"),
            P(("outer", "dp")),
            P(("outer", "dp"), None),
            P(("outer", "dp")),
            P(),
        ),
        out_specs=(P(), P(("outer", "dp"), "tensor"), P("tensor"), P("tensor")),
        check_vma=False,
    )
```
